64 devices in a mesh: dp: 8 (over x, y, core), tp: 8 (over z).
Axes of the slice: x: 2, y: 2, z: 8, core: 2. Of those that a mesh axis runs over, the one named last changes fastest.
The devices are a block of a 4x4x8 slice.
Arguments:
- x: bfloat16 [16384, 1024], P('dp'), parts along dimension 0
- gain: bfloat16 [1024], replicated
- wq: bfloat16 [1024, 16384], P(None, 'tp')
- wk: bfloat16 [1024, 16384], P(None, 'tp')
- wv: bfloat16 [1024, 16384], P(None, 'tp')
- wo: bfloat16 [16384, 1024], P('tp')
Outputs:
- output: bfloat16 [16384, 1024], P('dp'), parts along dimension 0
There are 8 independent parts. The reference program is written for one: setup_inputs(seed, part) draws one part's arguments, and reference() takes and returns one part's arrays. A program takes and returns all parts, laid end to end along the dimension named above; an argument that names none is the same for every part.
All inputs are finite; a program needn't handle non-finite values.
Results may differ from the reference program's by a relative error of at most 0.012.
Values are sent between devices in bfloat16 or wider.
A program may use at most 768 MiB of HBM per device.

```python
import jax
import jax.numpy as jnp
from jax import lax

ROWS = 2048
D = 1024
HEADS = 128
KV_HEADS = 128
HEAD = 128
THETA = 10000


def setup_inputs(seed: int = 0, part: int = 0) -> dict:
    kx, kn, kq, kk, kv, ko = jax.random.split(jax.random.key(seed), 6)

    def weights(key, rows, columns):
        return jax.random.normal(key, (rows, columns), jnp.float32) * rows**-0.5

    drawn = {
        "x": jax.random.normal(jax.random.fold_in(kx, part), (ROWS, D), jnp.float32),
        "gain": 1 + 0.1 * jax.random.normal(kn, (D,), jnp.float32),
        "wq": 2 * weights(kq, D, HEADS * HEAD),
        "wk": 2 * weights(kk, D, KV_HEADS * HEAD),
        "wv": 4 * weights(kv, D, KV_HEADS * HEAD),
        "wo": weights(ko, HEADS * HEAD, D),
    }
    return {k: v.astype(jnp.bfloat16) for k, v in drawn.items()}


def normed(x, gain):
    wide = x.astype(jnp.float32)
    scale = lax.rsqrt(jnp.mean(wide * wide, -1, keepdims=True) + 1e-6)
    return (wide * scale * gain.astype(jnp.float32)).astype(jnp.bfloat16)


def turned(t, place, theta):
    half = t.shape[-1] // 2
    angle = place.astype(jnp.float32)[:, None] * theta ** (-jnp.arange(half, dtype=jnp.float32) / half)
    cos, sin = jnp.cos(angle)[:, None], jnp.sin(angle)[:, None]
    a, b = t[..., :half].astype(jnp.float32), t[..., half:].astype(jnp.float32)
    return jnp.concatenate([a * cos - b * sin, b * cos + a * sin], -1).astype(jnp.bfloat16)


def matmul(a, w):
    return jnp.dot(a, w, preferred_element_type=jnp.float32).astype(jnp.bfloat16)


def einsum(form, a, b):
    return jnp.einsum(form, a.astype(jnp.float32), b.astype(jnp.float32))


def attention(q, k, v):
    scores = einsum("tgsd,ugd->gstu", q, k) * q.shape[-1] ** -0.5
    token = jnp.arange(q.shape[0])
    scores = jnp.where(token[:, None] >= token, scores, -jnp.inf)
    weights = jax.nn.softmax(scores, -1).astype(jnp.bfloat16)
    return einsum("gstu,ugd->tgsd", weights, v).astype(jnp.bfloat16)


def reference(x, gain, wq, wk, wv, wo):
    a, place = normed(x, gain), jnp.arange(ROWS)
    q = turned(matmul(a, wq).reshape(ROWS, HEADS, HEAD), place, THETA).reshape(ROWS, KV_HEADS, -1, HEAD)
    k = turned(matmul(a, wk).reshape(ROWS, KV_HEADS, HEAD), place, THETA)
    v = matmul(a, wv).reshape(ROWS, KV_HEADS, HEAD)
    seen = attention(q, k, v).reshape(ROWS, HEADS * HEAD)
    return (x.astype(jnp.float32) + jnp.dot(seen, wo, preferred_element_type=jnp.float32)).astype(jnp.bfloat16)
```

```python
import functools

import numpy as np
import jax
import jax.numpy as jnp
from jax import lax
from jax.experimental import pallas as pl
from jax.experimental.pallas import tpu as pltpu
from jax.sharding import PartitionSpec as P

HEAD = 128
THETA = 10000
R = 256
NEG = -1e30
HIDDEN = 2 * NEG
LOG2E = 1.4426950408889634
ONES = 16
VMEM = 62 * 2**20


def _dot(a, b, ca, cb):
    return lax.dot_general(a, b, (((ca,), (cb,)), ((), ())), preferred_element_type=jnp.float32)


def _tables(rows):
    half = HEAD // 2
    step = np.float32(THETA) ** (-np.arange(half, dtype=np.float32) / np.float32(half))
    angle = (np.arange(rows, dtype=np.float32)[:, None] * step).astype(np.float32)
    cos, sin = np.cos(angle).astype(np.float32), np.sin(angle).astype(np.float32)
    return np.concatenate([cos, cos], 1), np.concatenate([-sin, sin], 1)


def kernel(x_ref, gain_ref, cos_ref, sin_ref, wq_hbm, wk_hbm, wv_hbm, wo_hbm, y_ref,
           wq, wk, wv, wo, xn, q_s, k_s, v_s, s_s, top, keep, acc, o_s, sems):
    c = pl.program_id(0)
    heads = q_s.shape[0]
    e = HEAD**-0.5 * LOG2E
    loads = [pltpu.make_async_copy(a, b, sems.at[i]) for i, (a, b) in enumerate([(wq_hbm, wq), (wk_hbm, wk), (wv_hbm, wv), (wo_hbm, wo)])]

    @pl.when(c == 0)
    def _():
        for d in loads:
            d.start()
        v_s[:, HEAD:, :] = jnp.ones((heads, ONES, v_s.shape[2]), v_s.dtype)

    wide = x_ref[...].astype(jnp.float32)
    scale = lax.rsqrt(jnp.mean(wide * wide, -1, keepdims=True) + 1e-6)
    xn[...] = (wide * scale * gain_ref[...].astype(jnp.float32)).astype(xn.dtype)
    here = pl.ds(pl.multiple_of(c * R, R), R)

    def turn(t):
        t = t.astype(jnp.bfloat16).astype(jnp.float32)
        return (t * cos_ref[...] + pltpu.roll(t, HEAD // 2, 1) * sin_ref[...]).astype(jnp.bfloat16)

    def project(i, w, put):
        @pl.when(c == 0)
        def _():
            loads[i].wait()

        for n in range(heads // 2):
            both = _dot(xn[...], w[:, n * 2 * HEAD : (n + 1) * 2 * HEAD], 1, 0)
            put(n, both)

    def put_q(n, t):
        for m in range(2):
            q_s[2 * n + m] = turn(t[:, m * HEAD : (m + 1) * HEAD])

    def put_k(n, t):
        for m in range(2):
            k_s[2 * n + m, here, :] = turn(t[:, m * HEAD : (m + 1) * HEAD])

    def put_v(n, t):
        t = t.astype(jnp.bfloat16).T
        for m in range(2):
            v_s[2 * n + m, :HEAD, here] = t[m * HEAD : (m + 1) * HEAD, :]

    project(0, wq, put_q)
    project(1, wk, put_k)
    project(2, wv, put_v)

    def score(h, j, first):
        keys = pl.ds(pl.multiple_of(j * R, R), R)
        s = _dot(k_s[h, keys, :], q_s[h], 1, 1)
        if first:
            ok = lax.broadcasted_iota(jnp.int32, (R, R), 1) >= lax.broadcasted_iota(jnp.int32, (R, R), 0)
            s = jnp.where(ok, s, HIDDEN)
        high = jnp.broadcast_to(s.reshape(R // 8, 8, R).max(0).max(0, keepdims=True), (8, R))
        if first:
            top[h] = high
        else:
            old = top[h]
            new = jnp.maximum(old, high)
            top[h] = new
            keep[h] = jnp.exp2((old - new) * e)
        s_s[h] = s

    def weigh(h, j, first):
        keys = pl.ds(pl.multiple_of(j * R, R), R)
        p = jnp.exp2((s_s[h].reshape(R // 8, 8, R) - top[h][None]) * e).reshape(R, R).astype(jnp.bfloat16)
        return _dot(v_s[h, :, keys], p, 1, 0)[: HEAD + 8]

    for h in range(heads):
        score(h, c, True)

    def add(h, j, first):
        mixed = weigh(h, j, first)

        if first:
            acc[h] = mixed
        else:
            acc[h] = (acc[h].reshape(-1, 8, R) * keep[h][None]).reshape(-1, R) + mixed

    @pl.when(c > 0)
    def _():
        for h in range(heads):
            add(h, c, True)
            score(h, 0, False)

        def body(j, _):
            for h in range(heads):
                add(h, j - 1, False)
                score(h, j, False)

        lax.fori_loop(1, c, body, None)
        for h in range(heads):
            add(h, c - 1, False)

    @pl.when(c == 0)
    def _():
        for h in range(heads):
            add(h, c, True)

    for h in range(heads):
        a = acc[h]
        o = (a[:HEAD].reshape(-1, 8, R) * (1 / a[HEAD:])[None]).reshape(HEAD, R).astype(jnp.bfloat16)
        o_s[:, h * HEAD : (h + 1) * HEAD] = o.T

    @pl.when(c == 0)
    def _():
        loads[3].wait()

    y_ref[...] = _dot(o_s[...], wo[...], 1, 0).astype(y_ref.dtype)


def fused(x, gain, wq, wk, wv, wo):
    rows, d = x.shape
    heads = wq.shape[1] // HEAD
    cos, sin = _tables(rows)
    row = lambda c: (c, 0)
    any_ = pl.BlockSpec(memory_space=pl.ANY)
    low = jnp.bfloat16
    return pl.pallas_call(
        kernel,
        grid=(rows // R,),
        in_specs=[pl.BlockSpec((R, d), row), pl.BlockSpec((1, d), lambda c: (0, 0)), pl.BlockSpec((R, HEAD), row), pl.BlockSpec((R, HEAD), row),
                  any_, any_, any_, any_],
        out_specs=pl.BlockSpec((R, d), row),
        out_shape=jax.ShapeDtypeStruct((rows, d), low),
        scratch_shapes=[
            pltpu.VMEM(wq.shape, low), pltpu.VMEM(wk.shape, low), pltpu.VMEM(wv.shape, low), pltpu.VMEM(wo.shape, low),
            pltpu.VMEM((R, d), low),
            pltpu.VMEM((heads, R, HEAD), low),
            pltpu.VMEM((heads, rows, HEAD), low),
            pltpu.VMEM((heads, HEAD + ONES, rows), low),
            pltpu.VMEM((heads, R, R), jnp.float32),
            pltpu.VMEM((heads, 8, R), jnp.float32),
            pltpu.VMEM((heads, 8, R), jnp.float32),
            pltpu.VMEM((heads, HEAD + 8, R), jnp.float32),
            pltpu.VMEM((R, heads * HEAD), low),
            pltpu.SemaphoreType.DMA((4,)),
        ],
        compiler_params=pltpu.CompilerParams(dimension_semantics=("arbitrary",), vmem_limit_bytes=VMEM),
        name="fused",
    )(x, gain.reshape(1, d), jnp.asarray(cos), jnp.asarray(sin), wq, wk, wv, wo)


def solution(mesh):
    def step(x, gain, wq, wk, wv, wo):
        term = fused(x, gain, wq, wk, wv, wo)
        y = lax.psum(term, "tp")
        return (x.astype(jnp.float32) + y.astype(jnp.float32)).astype(jnp.bfloat16)

    tokens, columns = P("dp", None), P(None, "tp")
    return jax.shard_map(
        step,
        mesh=mesh,
        in_specs=(tokens, P(None), columns, columns, columns, P("tp", None)),
        out_specs=tokens,
        check_vma=False,
    )
```

```python
import functools

import numpy as np
import jax
import jax.numpy as jnp
from jax import lax
from jax.experimental import pallas as pl
from jax.experimental.pallas import tpu as pltpu
from jax.sharding import PartitionSpec as P

HEAD = 128
THETA = 10000
R = 256
NEG = -1e30
HIDDEN = 2 * NEG
LOG2E = 1.4426950408889634
ONES = 16
PARTS = 2
PLACES = 8
SPACE = 3
VMEM = 62 * 2**20


def _dot(a, b, ca, cb):
    return lax.dot_general(a, b, (((ca,), (cb,)), ((), ())), preferred_element_type=jnp.float32)


def _table(rows):
    half = HEAD // 2
    step = np.float32(THETA) ** (-np.arange(half, dtype=np.float32) / np.float32(half))
    angle = (np.arange(rows, dtype=np.float32)[:, None] * step).astype(np.float32)
    return np.concatenate([np.cos(angle), np.sin(angle)], 1).astype(np.float32)


def kernel(n, x_ref, gain_ref, tab_ref, wq_hbm, wk_hbm, wv_hbm, wo_hbm, y_hbm,
           wq, wk, wv, wo, xn, cos_s, sin_s, q_s, k_s, v_s, s_s, top, keep, acc, o_s, term, snd, got, y_v,
           sems, rs_send, rs_recv, ag_send, ag_recv, out_sem):
    c = pl.program_id(0)
    blocks = pl.num_programs(0)
    heads = q_s.shape[0]
    e = HEAD**-0.5 * LOG2E
    loads = [pltpu.make_async_copy(a, b, sems.at[i]) for i, (a, b) in enumerate([(wq_hbm, wq), (wk_hbm, wk), (wv_hbm, wv), (wo_hbm, wo)])]

    me = lax.axis_index("tp")
    right, left = lax.rem(me + 1, n), lax.rem(me + n - 1, n)
    far, near = n // 2, n - 1 - n // 2
    S = R // n

    def owner(k):
        return lax.rem(me + (k + n), n)

    def slice_of(k):
        return pl.ds(pl.multiple_of(owner(k) * S, S), S)

    def part(k, g):
        return pl.ds(pl.multiple_of(owner(k) * S + g * (S // PARTS), S // PARTS), S // PARTS)

    def send_term(b, i, g):
        two = lax.rem(b, 2)
        return pltpu.make_async_remote_copy(src_ref=snd.at[two, i, g], dst_ref=got.at[b, i, g], send_sem=rs_send.at[two, i, g], recv_sem=rs_recv.at[b, i, g],
                                            device_id={"tp": right if i < far else left}, device_id_type=pl.DeviceIdType.MESH)

    def send_done(b, i, g):
        k = -i if i < near else i - near
        size = S // PARTS
        rows = y_v.at[pl.ds(pl.multiple_of(b * R + owner(k) * S + g * size, size), size)]
        return pltpu.make_async_remote_copy(src_ref=rows, dst_ref=rows, send_sem=ag_send.at[lax.rem(b, 2), i, g], recv_sem=ag_recv.at[b, i, g],
                                            device_id={"tp": right if i < near else left}, device_id_type=pl.DeviceIdType.MESH)

    def write_out(b):
        rows = pl.ds(pl.multiple_of(b * R, R), R)
        return pltpu.make_async_copy(y_v.at[rows], y_hbm.at[rows], out_sem.at[b])

    def pass_term(b, i, k, g):
        two = lax.rem(b, 2)
        mine = term[two, part(k, g), :]
        if i not in (0, far):
            send_term(b, i - 1, g).wait_recv()
            mine = got[b, i - 1, g].astype(jnp.float32) + mine
        snd[two, i, g] = mine.astype(snd.dtype)
        send_term(b, i, g).start()

    def start_terms(b):
        for g in range(PARTS):
            pass_term(b, 0, far, g)
            pass_term(b, far, -near, g)

    def reduce_step(b, i):
        for g in range(PARTS):
            if i < far - 1:
                pass_term(b, i + 1, far - 1 - i, g)
            if i < near - 1:
                pass_term(b, far + i + 1, i + 1 - near, g)
            if i == far - 1:
                send_term(b, far - 1, g).wait_recv()
                send_term(b, n - 2, g).wait_recv()
                total = got[b, far - 1, g].astype(jnp.float32) + got[b, n - 2, g].astype(jnp.float32) + term[lax.rem(b, 2), part(0, g), :]
                size = S // PARTS
                y_v[pl.ds(pl.multiple_of(b * R + me * S + g * size, size), size), :] = total.astype(y_v.dtype)
                send_done(b, 0, g).start()
                send_done(b, near, g).start()
        if i == far - 1:
            for k in range(n - 1):
                for g in range(PARTS):
                    send_term(b, k, g).wait_send()

    def gather_step(b, i):
        for g in range(PARTS):
            if i < near:
                send_done(b, i, g).wait_recv()
                if i + 1 < near:
                    send_done(b, i + 1, g).start()
            send_done(b, near + i, g).wait_recv()
            if i + 1 < far:
                send_done(b, near + i + 1, g).start()
        if i == far - 1:
            for k in range(n - 1):
                for g in range(PARTS):
                    send_done(b, k, g).wait_send()
            write_out(b).start()

    def due(p):
        for m in range(1, 2 + SPACE * 2 * far // PLACES):
            k, off = divmod(PLACES * (m - 1) + p - (SPACE - 1), SPACE)
            if off == 0 and 0 <= k < 2 * far:
                yield m, k

    def take(b, k):
        if k < far:
            reduce_step(b, k)
        else:
            gather_step(b, k - far)

    def tick(p):
        for m, k in due(p):
            @pl.when(c >= m)
            def _():
                take(c - m, k)

    @pl.when(c == 0)
    def _():
        barrier = pltpu.get_barrier_semaphore()
        for d in (left, right):
            pl.semaphore_signal(barrier, inc=1, device_id={"tp": d}, device_id_type=pl.DeviceIdType.MESH)
        for d in loads:
            d.start()
        v_s[:, HEAD:, :] = jnp.ones((heads, ONES, v_s.shape[2]), v_s.dtype)
        pl.semaphore_wait(barrier, 2)

    wide = x_ref[...].astype(jnp.float32)
    scale = lax.rsqrt(jnp.mean(wide * wide, -1, keepdims=True) + 1e-6)
    xn[...] = (wide * scale * gain_ref[...].astype(jnp.float32)).astype(xn.dtype)
    here = pl.ds(pl.multiple_of(c * R, R), R)
    tab = tab_ref[...]
    swapped = pltpu.roll(tab, HEAD // 2, 1)
    low_half = lax.broadcasted_iota(jnp.int32, tab.shape, 1) < HEAD // 2
    cos_s[...] = jnp.where(low_half, tab, swapped)
    sin_s[...] = jnp.where(low_half, -swapped, tab)

    def turn(t):
        t = t.astype(jnp.bfloat16).astype(jnp.float32)
        return (t * cos_s[...] + pltpu.roll(t, HEAD // 2, 1) * sin_s[...]).astype(jnp.bfloat16)

    def project(i, w, put):
        @pl.when(c == 0)
        def _():
            loads[i].wait()

        for m in range(heads // 2):
            put(m, _dot(xn[...], w[:, m * 2 * HEAD : (m + 1) * 2 * HEAD], 1, 0))

    def put_q(i, t):
        for m in range(2):
            q_s[2 * i + m] = turn(t[:, m * HEAD : (m + 1) * HEAD])

    def put_k(i, t):
        for m in range(2):
            k_s[2 * i + m, here, :] = turn(t[:, m * HEAD : (m + 1) * HEAD])

    def put_v(i, t):
        t = t.astype(jnp.bfloat16).T
        for m in range(2):
            v_s[2 * i + m, :HEAD, here] = t[m * HEAD : (m + 1) * HEAD, :]

    def score(h, j, first):
        keys = pl.ds(pl.multiple_of(j * R, R), R)
        s = _dot(k_s[h, keys, :], q_s[h], 1, 1)
        if first:
            ok = lax.broadcasted_iota(jnp.int32, (R, R), 1) >= lax.broadcasted_iota(jnp.int32, (R, R), 0)
            s = jnp.where(ok, s, HIDDEN)
        high = jnp.broadcast_to(s.reshape(R // 8, 8, R).max(0).max(0, keepdims=True), (8, R))
        if first:
            top[h] = high
        else:
            old = top[h]
            new = jnp.maximum(old, high)
            top[h] = new
            keep[h] = jnp.exp2((old - new) * e)
        s_s[h] = s

    def add(h, j, first):
        keys = pl.ds(pl.multiple_of(j * R, R), R)
        p = jnp.exp2((s_s[h].reshape(R // 8, 8, R) - top[h][None]) * e).reshape(R, R).astype(jnp.bfloat16)
        mixed = _dot(v_s[h, :, keys], p, 1, 0)[: HEAD + 8]
        acc[h] = mixed if first else (acc[h].reshape(-1, 8, R) * keep[h][None]).reshape(-1, R) + mixed

    def body(j, _):
        for h in range(heads):
            add(h, j - 1, False)
            score(h, j, False)

    project(0, wq, put_q)
    tick(0)
    project(1, wk, put_k)
    tick(1)
    project(2, wv, put_v)
    for h in range(heads):
        score(h, c, True)
    tick(2)

    @pl.when(c > 0)
    def _():
        for h in range(heads):
            add(h, c, True)
            score(h, 0, False)
        tick(3)
        third, most = 1 + lax.div(c - 1, 3), 1 + lax.div(2 * (c - 1), 3)
        lax.fori_loop(1, third, body, None)
        tick(4)
        lax.fori_loop(third, most, body, None)
        tick(5)
        lax.fori_loop(most, c, body, None)
        for h in range(heads):
            add(h, c - 1, False)
        tick(6)

    @pl.when(c == 0)
    def _():
        for h in range(heads):
            add(h, c, True)

    for h in range(heads):
        a = acc[h]
        o = (a[:HEAD].reshape(-1, 8, R) * (1 / a[HEAD:])[None]).reshape(HEAD, R).astype(jnp.bfloat16)
        o_s[:, h * HEAD : (h + 1) * HEAD] = o.T
    tick(7)

    @pl.when(c == 0)
    def _():
        loads[3].wait()

    two = lax.rem(c, 2)
    term[two] = _dot(o_s[...], wo[...], 1, 0)
    mine = pl.ds(pl.multiple_of(me * S, S), S)
    term[two, mine, :] = term[two, mine, :] + x_ref[mine, :].astype(jnp.float32)
    start_terms(c)

    @pl.when(c == blocks - 1)
    def _():
        for late in range(1, 5):
            for p in range(PLACES):
                for m, k in due(p):
                    if m >= late:
                        take(c + late - m, k)
        lax.fori_loop(0, blocks, lambda b, _: write_out(b).wait(), None)


def fused(n, x, gain, wq, wk, wv, wo):
    rows, d = x.shape
    heads, blocks = wq.shape[1] // HEAD, rows // R
    row = lambda c: (c, 0)
    any_ = pl.BlockSpec(memory_space=pl.ANY)
    low = jnp.bfloat16
    dma = pltpu.SemaphoreType.DMA
    return pl.pallas_call(
        functools.partial(kernel, n),
        grid=(blocks,),
        in_specs=[pl.BlockSpec((R, d), row), pl.BlockSpec((1, d), lambda c: (0, 0)), pl.BlockSpec((R, HEAD), row), any_, any_, any_, any_],
        out_specs=any_,
        out_shape=jax.ShapeDtypeStruct((rows, d), low),
        scratch_shapes=[
            pltpu.VMEM(wq.shape, low), pltpu.VMEM(wk.shape, low), pltpu.VMEM(wv.shape, low), pltpu.VMEM(wo.shape, low),
            pltpu.VMEM((R, d), low),
            pltpu.VMEM((R, HEAD), jnp.float32), pltpu.VMEM((R, HEAD), jnp.float32),
            pltpu.VMEM((heads, R, HEAD), low),
            pltpu.VMEM((heads, rows, HEAD), low),
            pltpu.VMEM((heads, HEAD + ONES, rows), low),
            pltpu.VMEM((heads, R, R), jnp.float32),
            pltpu.VMEM((heads, 8, R), jnp.float32),
            pltpu.VMEM((heads, 8, R), jnp.float32),
            pltpu.VMEM((heads, HEAD + 8, R), jnp.float32),
            pltpu.VMEM((R, heads * HEAD), low),
            pltpu.VMEM((2, R, d), jnp.float32),
            pltpu.VMEM((2, n - 1, PARTS, R // n // PARTS, d), low),
            pltpu.VMEM((blocks, n - 1, PARTS, R // n // PARTS, d), low),
            pltpu.VMEM((rows, d), low),
            dma((4,)), dma((2, n - 1, PARTS)), dma((blocks, n - 1, PARTS)), dma((2, n - 1, PARTS)), dma((blocks, n - 1, PARTS)), dma((blocks,)),
        ],
        compiler_params=pltpu.CompilerParams(dimension_semantics=("arbitrary",), vmem_limit_bytes=VMEM, collective_id=0, has_side_effects=True),
        name="fused",
    )(x, gain.reshape(1, d), jnp.asarray(_table(rows)), wq, wk, wv, wo)


def solution(mesh):
    def step(x, gain, wq, wk, wv, wo):
        return fused(mesh.shape["tp"], x, gain, wq, wk, wv, wo)

    tokens, columns = P("dp", None), P(None, "tp")
    return jax.shard_map(
        step,
        mesh=mesh,
        in_specs=(tokens, P(None), columns, columns, columns, P("tp", None)),
        out_specs=tokens,
        check_vma=False,
    )
```

```python
import functools

import numpy as np
import jax
import jax.numpy as jnp
from jax import lax
from jax.experimental import pallas as pl
from jax.experimental.pallas import tpu as pltpu
from jax.sharding import PartitionSpec as P

HEAD = 128
THETA = 10000
R = 256
NEG = -1e30
HIDDEN = 2 * NEG
LOG2E = 1.4426950408889634
ONES = 16
PARTS = 2
CUTS = 5
PLACES = CUTS + 3
SLOTS = 3
WIRE, TRIP, SPARE = 1.4, 2.3, 0.4
VMEM = 62 * 2**20


def _dot(a, b, ca, cb):
    return lax.dot_general(a, b, (((ca,), (cb,)), ((), ())), preferred_element_type=jnp.float32)


def _plan(blocks, steps):
    nexts, ready, link, now = [], [], 0.0, 0.0
    placed, tail = {}, []

    def run(b, k, at):
        nonlocal link
        assert k != steps // 2 - 1 or b < SLOTS or nexts[b - SLOTS] == steps
        if k < steps - 1:
            link = max(link, at) + WIRE
        nexts[b] = k + 1
        ready[b] = link + TRIP

    for c in range(blocks):
        runs = [1.1 * ((i + 1) * (c - 1) // CUTS - i * (c - 1) // CUTS) for i in range(CUTS)]
        gaps = [1.45, 1.95, 1.1, *runs[:-1], runs[-1] + (1.8 if c < blocks - 1 else 1.1)] if c else [4.5, 1.95, *[0] * CUTS, 1.7]
        for p in range(PLACES):
            now += gaps[p]
            for b in range(len(nexts)):
                must = p == PLACES - 1 and b == c - SLOTS and nexts[b] <= steps // 2 - 1
                while nexts[b] < steps and (ready[b] + SPARE <= now or must):
                    now = max(now, ready[b])
                    placed.setdefault((p, c - b, nexts[b]), []).append(c)
                    run(b, nexts[b], now)
                    must = must and nexts[b] <= steps // 2 - 1
        now += 1.5
        nexts.append(0), ready.append(0.0)
        run(c, -1, now)
    while min(nexts) < steps:
        b = min((b for b in range(blocks) if nexts[b] < steps), key=lambda b: ready[b] - (b == blocks - 1))
        now = max(now, ready[b])
        tail.append((b, nexts[b]))
        run(b, nexts[b], now)
    return placed, tail


def _table(rows):
    half = HEAD // 2
    step = np.float32(THETA) ** (-np.arange(half, dtype=np.float32) / np.float32(half))
    angle = (np.arange(rows, dtype=np.float32)[:, None] * step).astype(np.float32)
    return np.concatenate([np.cos(angle), np.sin(angle)], 1).astype(np.float32)


def kernel(n, count, x_ref, x_next, gain_ref, tab_ref, tab_next, wq_hbm, wk_hbm, wv_hbm, wo_hbm, y_hbm,
           wq, wk, wv, wo, xn, cos_s, sin_s, q_s, k_s, v_s, s_s, top, keep, acc, o_s, term, snd, got, y_v,
           sems, rs_send, rs_recv, ag_send, ag_recv, out_sem):
    c = pl.program_id(0)
    blocks = pl.num_programs(0)
    heads = q_s.shape[0]
    e = HEAD**-0.5 * LOG2E
    loads = [pltpu.make_async_copy(a, b, sems.at[i]) for i, (a, b) in enumerate([(wq_hbm, wq), (wk_hbm, wk), (wv_hbm, wv), (wo_hbm, wo)])]

    me = lax.axis_index("tp")
    right, left = lax.rem(me + 1, n), lax.rem(me + n - 1, n)
    far, near = n // 2, n - 1 - n // 2
    S = R // n

    def owner(k):
        return lax.rem(me + (k + n), n)

    def slice_of(k):
        return pl.ds(pl.multiple_of(owner(k) * S, S), S)

    def part(k, g):
        return pl.ds(pl.multiple_of(owner(k) * S + g * (S // PARTS), S // PARTS), S // PARTS)

    def send_term(b, i, g):
        slot = lax.rem(b, SLOTS)
        return pltpu.make_async_remote_copy(src_ref=snd.at[slot, i, g], dst_ref=got.at[b, i, g], send_sem=rs_send.at[slot, i, g], recv_sem=rs_recv.at[b, i, g],
                                            device_id={"tp": right if i < far else left}, device_id_type=pl.DeviceIdType.MESH)

    def send_done(b, i, g):
        k = -i if i < near else i - near
        size = S // PARTS
        rows = y_v.at[pl.ds(pl.multiple_of(b * R + owner(k) * S + g * size, size), size)]
        return pltpu.make_async_remote_copy(src_ref=rows, dst_ref=rows, send_sem=ag_send.at[lax.rem(b, SLOTS), i, g], recv_sem=ag_recv.at[b, i, g],
                                            device_id={"tp": right if i < near else left}, device_id_type=pl.DeviceIdType.MESH)

    def write_out(b):
        rows = pl.ds(pl.multiple_of(b * R, R), R)
        return pltpu.make_async_copy(y_v.at[rows], y_hbm.at[rows], out_sem.at[b])

    def pass_term(b, i, k, g):
        slot = lax.rem(b, SLOTS)
        mine = term[slot, part(k, g), :]
        if i not in (0, far):
            send_term(b, i - 1, g).wait_recv()
            mine = got[b, i - 1, g].astype(jnp.float32) + mine
        snd[slot, i, g] = mine.astype(snd.dtype)
        send_term(b, i, g).start()

    def start_terms(b):
        for g in range(PARTS):
            pass_term(b, 0, far, g)
            pass_term(b, far, -near, g)

    def reduce_step(b, i):
        for g in range(PARTS):
            if i < far - 1:
                pass_term(b, i + 1, far - 1 - i, g)
            if i < near - 1:
                pass_term(b, far + i + 1, i + 1 - near, g)
            if i == far - 1:
                send_term(b, far - 1, g).wait_recv()
                send_term(b, n - 2, g).wait_recv()
                total = got[b, far - 1, g].astype(jnp.float32) + got[b, n - 2, g].astype(jnp.float32) + term[lax.rem(b, SLOTS), part(0, g), :]
                size = S // PARTS
                y_v[pl.ds(pl.multiple_of(b * R + me * S + g * size, size), size), :] = total.astype(y_v.dtype)
                send_done(b, 0, g).start()
                send_done(b, near, g).start()
        if i == far - 1:
            for k in range(n - 1):
                for g in range(PARTS):
                    send_term(b, k, g).wait_send()

    def gather_step(b, i):
        for g in range(PARTS):
            if i < near:
                send_done(b, i, g).wait_recv()
                if i + 1 < near:
                    send_done(b, i + 1, g).start()
            send_done(b, near + i, g).wait_recv()
            if i + 1 < far:
                send_done(b, near + i + 1, g).start()
        if i == far - 1:
            for k in range(n - 1):
                for g in range(PARTS):
                    send_done(b, k, g).wait_send()
            write_out(b).start()

    def take(b, k):
        if k < far:
            reduce_step(b, k)
        else:
            gather_step(b, k - far)

    placed, tail = _plan(count, 2 * far)

    def tick(p):
        for m, k in sorted({(m, k) for q, m, k in placed if q == p}, key=lambda mk: (-mk[0], mk[1])):
            at = placed[p, m, k]
            when = functools.reduce(lambda a, b: a | b, [c == b for b in at]) if at != list(range(at[0], at[-1] + 1)) else (c >= at[0]) & (c <= at[-1])

            @pl.when(when)
            def _():
                take(c - m, k)

    @pl.when(c == 0)
    def _():
        barrier = pltpu.get_barrier_semaphore()
        for d in (left, right):
            pl.semaphore_signal(barrier, inc=1, device_id={"tp": d}, device_id_type=pl.DeviceIdType.MESH)
        for d in loads:
            d.start()
        v_s[:, HEAD:, :] = jnp.ones((heads, ONES, v_s.shape[2]), v_s.dtype)
        pl.semaphore_wait(barrier, 2)

    here = pl.ds(pl.multiple_of(c * R, R), R)

    def prepare(x, tab):
        wide = x[...].astype(jnp.float32)
        scale = lax.rsqrt(jnp.mean(wide * wide, -1, keepdims=True) + 1e-6)
        xn[...] = (wide * scale * gain_ref[...].astype(jnp.float32)[None]).astype(xn.dtype)
        tab = tab[...]
        swapped = pltpu.roll(tab, HEAD // 2, 1)
        low_half = lax.broadcasted_iota(jnp.int32, tab.shape, 1) < HEAD // 2
        cos_s[...] = jnp.where(low_half, tab, swapped)
        sin_s[...] = jnp.where(low_half, -swapped, tab)

    def turn(t):
        t = t.astype(jnp.bfloat16).astype(jnp.float32)
        return (t * cos_s[...] + pltpu.roll(t, HEAD // 2, 1) * sin_s[...]).astype(jnp.bfloat16)

    def project(m, w, put):
        put(m, _dot(xn[...], w[:, m * 2 * HEAD : (m + 1) * 2 * HEAD], 1, 0))

    def put_q(i, t):
        for m in range(2):
            q_s[2 * i + m] = turn(t[:, m * HEAD : (m + 1) * HEAD])

    def put_k(i, t):
        for m in range(2):
            k_s[2 * i + m, here, :] = turn(t[:, m * HEAD : (m + 1) * HEAD])

    def put_v(i, t):
        t = t.astype(jnp.bfloat16).T
        for m in range(2):
            v_s[2 * i + m, :HEAD, here] = t[m * HEAD : (m + 1) * HEAD, :]

    def score(h, j, first):
        keys = pl.ds(pl.multiple_of(j * R, R), R)
        s = _dot(k_s[h, keys, :], q_s[h], 1, 1)
        if first:
            ok = lax.broadcasted_iota(jnp.int32, (R, R), 1) >= lax.broadcasted_iota(jnp.int32, (R, R), 0)
            s = jnp.where(ok, s, HIDDEN)
        high = jnp.broadcast_to(s.reshape(R // 8, 8, R).max(0).max(0, keepdims=True), (8, R))
        if first:
            top[h] = high
        else:
            old = top[h]
            new = jnp.maximum(old, high)
            top[h] = new
            keep[h] = jnp.exp2((old - new) * e)
        s_s[h] = s

    def add(h, j, first):
        keys = pl.ds(pl.multiple_of(j * R, R), R)
        p = jnp.exp2((s_s[h].reshape(R // 8, 8, R) - top[h][None]) * e).reshape(R, R).astype(jnp.bfloat16)
        mixed = _dot(v_s[h, :, keys], p, 1, 0)[: HEAD + 8]
        acc[h] = mixed if first else (acc[h].reshape(-1, 8, R) * keep[h][None]).reshape(-1, R) + mixed

    def body(j, _):
        for h in range(heads):
            add(h, j - 1, False)
            score(h, j, False)

    def close(j, first, more):
        if more:
            prepare(x_next, tab_next)
        for m in range(heads // 2):
            if more:
                project(m, wq, put_q)
            for h in (2 * m, 2 * m + 1):
                add(h, j, first)
                a = acc[h]
                o = (a[:HEAD].reshape(-1, 8, R) * (1 / a[HEAD:])[None]).reshape(HEAD, R).astype(jnp.bfloat16)
                o_s[:, h * HEAD : (h + 1) * HEAD] = o.T

    @pl.when(c == 0)
    def _():
        prepare(x_ref, tab_ref)
        loads[0].wait()
        for m in range(heads // 2):
            project(m, wq, put_q)
        loads[1].wait()

    for m in range(heads // 2):
        project(m, wk, put_k)
    tick(0)

    @pl.when(c == 0)
    def _():
        loads[2].wait()

    for m in range(heads // 2):
        project(m, wv, put_v)
    for h in range(heads):
        score(h, c, True)
    tick(1)

    @pl.when(c > 0)
    def _():
        for h in range(heads):
            add(h, c, True)
            score(h, 0, False)
        tick(2)
        for i in range(CUTS):
            cut = lambda i: 1 + lax.div(i * (c - 1), CUTS)
            lax.fori_loop(cut(i), cut(i + 1), body, None)
            if i < CUTS - 1:
                tick(3 + i)

        @pl.when(c < count - 1)
        def _():
            close(c - 1, False, True)

        @pl.when(c == count - 1)
        def _():
            close(c - 1, False, False)

    @pl.when(c == 0)
    def _():
        close(c, True, True)

    tick(CUTS + 2)

    @pl.when(c == 0)
    def _():
        loads[3].wait()

    slot = lax.rem(c, SLOTS)
    term[slot] = _dot(o_s[...], wo[...], 1, 0)
    mine = pl.ds(pl.multiple_of(me * S, S), S)
    term[slot, mine, :] = term[slot, mine, :] + x_ref[mine, :].astype(jnp.float32)
    start_terms(c)

    @pl.when(c == blocks - 1)
    def _():
        for b, k in tail:
            take(b, k)
        lax.fori_loop(0, blocks, lambda b, _: write_out(b).wait(), None)


def fused(n, x, gain, wq, wk, wv, wo):
    rows, d = x.shape
    heads, blocks = wq.shape[1] // HEAD, rows // R
    row = lambda c: (c, 0)
    after = lambda c: (jnp.minimum(c + 1, blocks - 1), 0)
    tab = jnp.asarray(_table(rows))
    any_ = pl.BlockSpec(memory_space=pl.ANY)
    low = jnp.bfloat16
    dma = pltpu.SemaphoreType.DMA
    return pl.pallas_call(
        functools.partial(kernel, n, blocks),
        grid=(blocks,),
        in_specs=[pl.BlockSpec((R, d), row), pl.BlockSpec((R, d), after), pl.BlockSpec((d,), lambda c: (0,)), pl.BlockSpec((R, HEAD), row),
                  pl.BlockSpec((R, HEAD), after), any_, any_, any_, any_],
        out_specs=any_,
        out_shape=jax.ShapeDtypeStruct((rows, d), low),
        scratch_shapes=[
            pltpu.VMEM(wq.shape, low), pltpu.VMEM(wk.shape, low), pltpu.VMEM(wv.shape, low), pltpu.VMEM(wo.shape, low),
            pltpu.VMEM((R, d), low),
            pltpu.VMEM((R, HEAD), jnp.float32), pltpu.VMEM((R, HEAD), jnp.float32),
            pltpu.VMEM((heads, R, HEAD), low),
            pltpu.VMEM((heads, rows, HEAD), low),
            pltpu.VMEM((heads, HEAD + ONES, rows), low),
            pltpu.VMEM((heads, R, R), jnp.float32),
            pltpu.VMEM((heads, 8, R), jnp.float32),
            pltpu.VMEM((heads, 8, R), jnp.float32),
            pltpu.VMEM((heads, HEAD + 8, R), jnp.float32),
            pltpu.VMEM((R, heads * HEAD), low),
            pltpu.VMEM((SLOTS, R, d), jnp.float32),
            pltpu.VMEM((SLOTS, n - 1, PARTS, R // n // PARTS, d), low),
            pltpu.VMEM((blocks, n - 1, PARTS, R // n // PARTS, d), low),
            pltpu.VMEM((rows, d), low),
            dma((4,)), dma((SLOTS, n - 1, PARTS)), dma((blocks, n - 1, PARTS)), dma((SLOTS, n - 1, PARTS)), dma((blocks, n - 1, PARTS)), dma((blocks,)),
        ],
        compiler_params=pltpu.CompilerParams(dimension_semantics=("arbitrary",), vmem_limit_bytes=VMEM, collective_id=0, has_side_effects=True),
        name="fused",
    )(x, x, gain, tab, tab, wq, wk, wv, wo)


def solution(mesh):
    def step(x, gain, wq, wk, wv, wo):
        return fused(mesh.shape["tp"], x, gain, wq, wk, wv, wo)

    tokens, columns = P("dp", None), P(None, "tp")
    return jax.shard_map(
        step,
        mesh=mesh,
        in_specs=(tokens, P(None), columns, columns, columns, P("tp", None)),
        out_specs=tokens,
        check_vma=False,
    )
```

```python
import functools

import numpy as np
import jax
import jax.numpy as jnp
from jax import lax
from jax.experimental import pallas as pl
from jax.experimental.pallas import tpu as pltpu
from jax.sharding import PartitionSpec as P

HEAD = 128
THETA = 10000
R = 256
NEG = -1e30
HIDDEN = 2 * NEG
LOG2E = 1.4426950408889634
ONES = 16
PARTS = 2
CUTS = 5
PLACES = CUTS + 3
SLOTS = 3
WIRE, TRIP, SPARE = 1.4, 2.4, 1.1
VMEM = 62 * 2**20


def _dot(a, b, ca, cb):
    return lax.dot_general(a, b, (((ca,), (cb,)), ((), ())), preferred_element_type=jnp.float32)


def _plan(blocks, steps):
    nexts, ready, link, now = [], [], 0.0, 0.0
    placed, tail = {}, []

    def run(b, k, at):
        nonlocal link
        assert k != steps // 2 - 1 or b <= SLOTS or nexts[b - SLOTS - 1] == steps
        if k < steps - 1:
            link = max(link, at) + WIRE
        nexts[b] = k + 1
        ready[b] = link + TRIP

    for c in range(blocks):
        runs = [1.1 * ((i + 1) * (c - 1) // CUTS - i * (c - 1) // CUTS) for i in range(CUTS)]
        gaps = [1.45, 1.95, 1.1, *runs[:-1], runs[-1] + (1.8 if c < blocks - 1 else 1.1)] if c else [4.5, 1.95, *[0] * CUTS, 1.7]
        for p in range(PLACES):
            now += gaps[p]
            for b in range(len(nexts)):
                must = p == PLACES - 1 and b == c - SLOTS and nexts[b] <= steps // 2 - 1
                while nexts[b] < steps and (ready[b] + SPARE <= now or must):
                    now = max(now, ready[b])
                    placed.setdefault((p, c - b, nexts[b]), []).append(c)
                    run(b, nexts[b], now)
                    must = must and nexts[b] <= steps // 2 - 1
        now += 1.5
        nexts.append(0), ready.append(0.0)
        run(c, -1, now)
    left = {b: nexts[b] for b in range(blocks - 1) if nexts[b] < steps}
    for k in range(steps):
        most = -(-sum(steps - at for at in left.values()) // (steps - k))
        for b in sorted(left, key=lambda b: left[b])[:most]:
            tail.append((b, left[b]))
            left[b] += 1
        left = {b: at for b, at in left.items() if at < steps}
        tail.append((blocks - 1, k))
    tail += [(b, k) for b in left for k in range(left[b], steps)]
    done = {}
    for b, k in tail:
        done[b] = k
        assert k != steps // 2 - 1 or b <= SLOTS or done.get(b - SLOTS - 1, steps - 1) == steps - 1
    return placed, tail


def _table(rows):
    half = HEAD // 2
    step = np.float32(THETA) ** (-np.arange(half, dtype=np.float32) / np.float32(half))
    angle = (np.arange(rows, dtype=np.float32)[:, None] * step).astype(np.float32)
    return np.concatenate([np.cos(angle), np.sin(angle)], 1).astype(np.float32)


def kernel(n, count, x_ref, x_next, gain_ref, tab_ref, tab_next, wq_hbm, wk_hbm, wv_hbm, wo_hbm, y_hbm,
           wq, wk, wv, wo, xn, cos_s, sin_s, q_s, k_s, v_s, s_s, top, keep, acc, o_s, term, snd, got, y_v,
           sems, rs_send, rs_recv, ag_send, ag_recv, out_sem):
    c = pl.program_id(0)
    blocks = pl.num_programs(0)
    heads = q_s.shape[0]
    e = HEAD**-0.5 * LOG2E
    loads = [pltpu.make_async_copy(a, b, sems.at[i]) for i, (a, b) in enumerate([(wq_hbm, wq), (wk_hbm, wk), (wv_hbm, wv), (wo_hbm, wo)])]

    me = lax.axis_index("tp")
    right, left = lax.rem(me + 1, n), lax.rem(me + n - 1, n)
    far, near = n // 2, n - 1 - n // 2
    S = R // n

    def owner(k):
        return lax.rem(me + (k + n), n)

    def slice_of(k):
        return pl.ds(pl.multiple_of(owner(k) * S, S), S)

    def part(k, g):
        return pl.ds(pl.multiple_of(owner(k) * S + g * (S // PARTS), S // PARTS), S // PARTS)

    def send_term(b, i, g):
        slot = lax.rem(b, SLOTS)
        return pltpu.make_async_remote_copy(src_ref=snd.at[slot, i, g], dst_ref=got.at[b, i, g], send_sem=rs_send.at[slot, i, g], recv_sem=rs_recv.at[b, i, g],
                                            device_id={"tp": right if i < far else left}, device_id_type=pl.DeviceIdType.MESH)

    def send_done(b, i, g):
        k = -i if i < near else i - near
        size = S // PARTS
        rows = y_v.at[pl.ds(pl.multiple_of(b * R + owner(k) * S + g * size, size), size)]
        return pltpu.make_async_remote_copy(src_ref=rows, dst_ref=rows, send_sem=ag_send.at[lax.rem(b, SLOTS + 1), i, g], recv_sem=ag_recv.at[b, i, g],
                                            device_id={"tp": right if i < near else left}, device_id_type=pl.DeviceIdType.MESH)

    def write_out(b):
        rows = pl.ds(pl.multiple_of(b * R, R), R)
        return pltpu.make_async_copy(y_v.at[rows], y_hbm.at[rows], out_sem.at[b])

    def pass_term(b, i, k, g):
        slot = lax.rem(b, SLOTS)
        mine = term[slot, part(k, g), :]
        if i not in (0, far):
            send_term(b, i - 1, g).wait_recv()
            mine = got[b, i - 1, g].astype(jnp.float32) + mine
        snd[slot, i, g] = mine.astype(snd.dtype)
        send_term(b, i, g).start()

    def start_terms(b):
        for g in range(PARTS):
            pass_term(b, 0, far, g)
            pass_term(b, far, -near, g)

    def reduce_step(b, i):
        for g in range(PARTS):
            if i < far - 1:
                pass_term(b, i + 1, far - 1 - i, g)
            if i < near - 1:
                pass_term(b, far + i + 1, i + 1 - near, g)
            if i == far - 1:
                send_term(b, far - 1, g).wait_recv()
                send_term(b, n - 2, g).wait_recv()
                total = got[b, far - 1, g].astype(jnp.float32) + got[b, n - 2, g].astype(jnp.float32) + term[lax.rem(b, SLOTS), part(0, g), :]
                size = S // PARTS
                y_v[pl.ds(pl.multiple_of(b * R + me * S + g * size, size), size), :] = total.astype(y_v.dtype)
                send_done(b, 0, g).start()
                send_done(b, near, g).start()
        if i == far - 1:
            for k in range(n - 1):
                for g in range(PARTS):
                    send_term(b, k, g).wait_send()

    def gather_step(b, i):
        for g in range(PARTS):
            if i < near:
                send_done(b, i, g).wait_recv()
                if i + 1 < near:
                    send_done(b, i + 1, g).start()
            send_done(b, near + i, g).wait_recv()
            if i + 1 < far:
                send_done(b, near + i + 1, g).start()
        if i == far - 1:
            for k in range(n - 1):
                for g in range(PARTS):
                    send_done(b, k, g).wait_send()
            write_out(b).start()

    def take(b, k):
        if k < far:
            reduce_step(b, k)
        else:
            gather_step(b, k - far)

    placed, tail = _plan(count, 2 * far)

    def tick(p):
        for m, k in sorted({(m, k) for q, m, k in placed if q == p}, key=lambda mk: (-mk[0], mk[1])):
            at = placed[p, m, k]
            when = functools.reduce(lambda a, b: a | b, [c == b for b in at]) if at != list(range(at[0], at[-1] + 1)) else (c >= at[0]) & (c <= at[-1])

            @pl.when(when)
            def _():
                take(c - m, k)

    @pl.when(c == 0)
    def _():
        barrier = pltpu.get_barrier_semaphore()
        for d in (left, right):
            pl.semaphore_signal(barrier, inc=1, device_id={"tp": d}, device_id_type=pl.DeviceIdType.MESH)
        for d in loads:
            d.start()
        v_s[:, HEAD:, :] = jnp.ones((heads, ONES, v_s.shape[2]), v_s.dtype)
        pl.semaphore_wait(barrier, 2)

    here = pl.ds(pl.multiple_of(c * R, R), R)

    def prepare(x, tab):
        wide = x[...].astype(jnp.float32)
        scale = lax.rsqrt(jnp.mean(wide * wide, -1, keepdims=True) + 1e-6)
        xn[...] = (wide * scale * gain_ref[...].astype(jnp.float32)[None]).astype(xn.dtype)
        tab = tab[...]
        swapped = pltpu.roll(tab, HEAD // 2, 1)
        low_half = lax.broadcasted_iota(jnp.int32, tab.shape, 1) < HEAD // 2
        cos_s[...] = jnp.where(low_half, tab, swapped)
        sin_s[...] = jnp.where(low_half, -swapped, tab)

    def turn(t):
        t = t.astype(jnp.bfloat16).astype(jnp.float32)
        return (t * cos_s[...] + pltpu.roll(t, HEAD // 2, 1) * sin_s[...]).astype(jnp.bfloat16)

    def project(m, w, put):
        put(m, _dot(xn[...], w[:, m * 2 * HEAD : (m + 1) * 2 * HEAD], 1, 0))

    def put_q(i, t):
        for m in range(2):
            q_s[2 * i + m] = turn(t[:, m * HEAD : (m + 1) * HEAD])

    def put_k(i, t):
        for m in range(2):
            k_s[2 * i + m, here, :] = turn(t[:, m * HEAD : (m + 1) * HEAD])

    def put_v(i, t):
        t = t.astype(jnp.bfloat16).T
        for m in range(2):
            v_s[2 * i + m, :HEAD, here] = t[m * HEAD : (m + 1) * HEAD, :]

    def score(h, j, first):
        keys = pl.ds(pl.multiple_of(j * R, R), R)
        s = _dot(k_s[h, keys, :], q_s[h], 1, 1)
        if first:
            ok = lax.broadcasted_iota(jnp.int32, (R, R), 1) >= lax.broadcasted_iota(jnp.int32, (R, R), 0)
            s = jnp.where(ok, s, HIDDEN)
        high = jnp.broadcast_to(s.reshape(R // 8, 8, R).max(0).max(0, keepdims=True), (8, R))
        if first:
            top[h] = high
        else:
            old = top[h]
            new = jnp.maximum(old, high)
            top[h] = new
            keep[h] = jnp.exp2((old - new) * e)
        s_s[h] = s

    def add(h, j, first):
        keys = pl.ds(pl.multiple_of(j * R, R), R)
        p = jnp.exp2((s_s[h].reshape(R // 8, 8, R) - top[h][None]) * e).reshape(R, R).astype(jnp.bfloat16)
        mixed = _dot(v_s[h, :, keys], p, 1, 0)[: HEAD + 8]
        acc[h] = mixed if first else (acc[h].reshape(-1, 8, R) * keep[h][None]).reshape(-1, R) + mixed

    def body(j, _):
        for h in range(heads):
            add(h, j - 1, False)
            score(h, j, False)

    def close(j, first, more):
        if more:
            prepare(x_next, tab_next)
        for m in range(heads // 2):
            if more:
                project(m, wq, put_q)
            for h in (2 * m, 2 * m + 1):
                add(h, j, first)
                a = acc[h]
                o = (a[:HEAD].reshape(-1, 8, R) * (1 / a[HEAD:])[None]).reshape(HEAD, R).astype(jnp.bfloat16)
                o_s[:, h * HEAD : (h + 1) * HEAD] = o.T

    @pl.when(c == 0)
    def _():
        prepare(x_ref, tab_ref)
        loads[0].wait()
        for m in range(heads // 2):
            project(m, wq, put_q)
        loads[1].wait()

    for m in range(heads // 2):
        project(m, wk, put_k)
    tick(0)

    @pl.when(c == 0)
    def _():
        loads[2].wait()

    for m in range(heads // 2):
        project(m, wv, put_v)
    for h in range(heads):
        score(h, c, True)
    tick(1)

    @pl.when(c > 0)
    def _():
        for h in range(heads):
            add(h, c, True)
            score(h, 0, False)
        tick(2)
        for i in range(CUTS):
            cut = lambda i: 1 + lax.div(i * (c - 1), CUTS)
            lax.fori_loop(cut(i), cut(i + 1), body, None)
            if i < CUTS - 1:
                tick(3 + i)

        @pl.when(c < count - 1)
        def _():
            close(c - 1, False, True)

        @pl.when(c == count - 1)
        def _():
            close(c - 1, False, False)

    @pl.when(c == 0)
    def _():
        close(c, True, True)

    tick(CUTS + 2)

    @pl.when(c == 0)
    def _():
        loads[3].wait()

    slot = lax.rem(c, SLOTS)
    term[slot] = _dot(o_s[...], wo[...], 1, 0)
    mine = pl.ds(pl.multiple_of(me * S, S), S)
    term[slot, mine, :] = term[slot, mine, :] + x_ref[mine, :].astype(jnp.float32)
    start_terms(c)

    @pl.when(c == blocks - 1)
    def _():
        for b, k in tail:
            take(b, k)
        lax.fori_loop(0, blocks, lambda b, _: write_out(b).wait(), None)


def fused(n, x, gain, wq, wk, wv, wo):
    rows, d = x.shape
    heads, blocks = wq.shape[1] // HEAD, rows // R
    row = lambda c: (c, 0)
    after = lambda c: (jnp.minimum(c + 1, blocks - 1), 0)
    tab = jnp.asarray(_table(rows))
    any_ = pl.BlockSpec(memory_space=pl.ANY)
    low = jnp.bfloat16
    dma = pltpu.SemaphoreType.DMA
    return pl.pallas_call(
        functools.partial(kernel, n, blocks),
        grid=(blocks,),
        in_specs=[pl.BlockSpec((R, d), row), pl.BlockSpec((R, d), after), pl.BlockSpec((d,), lambda c: (0,)), pl.BlockSpec((R, HEAD), row),
                  pl.BlockSpec((R, HEAD), after), any_, any_, any_, any_],
        out_specs=any_,
        out_shape=jax.ShapeDtypeStruct((rows, d), low),
        scratch_shapes=[
            pltpu.VMEM(wq.shape, low), pltpu.VMEM(wk.shape, low), pltpu.VMEM(wv.shape, low), pltpu.VMEM(wo.shape, low),
            pltpu.VMEM((R, d), low),
            pltpu.VMEM((R, HEAD), jnp.float32), pltpu.VMEM((R, HEAD), jnp.float32),
            pltpu.VMEM((heads, R, HEAD), low),
            pltpu.VMEM((heads, rows, HEAD), low),
            pltpu.VMEM((heads, HEAD + ONES, rows), low),
            pltpu.VMEM((heads, R, R), jnp.float32),
            pltpu.VMEM((heads, 8, R), jnp.float32),
            pltpu.VMEM((heads, 8, R), jnp.float32),
            pltpu.VMEM((heads, HEAD + 8, R), jnp.float32),
            pltpu.VMEM((R, heads * HEAD), low),
            pltpu.VMEM((SLOTS, R, d), jnp.float32),
            pltpu.VMEM((SLOTS, n - 1, PARTS, R // n // PARTS, d), low),
            pltpu.VMEM((blocks, n - 1, PARTS, R // n // PARTS, d), low),
            pltpu.VMEM((rows, d), low),
            dma((4,)), dma((SLOTS, n - 1, PARTS)), dma((blocks, n - 1, PARTS)), dma((SLOTS + 1, n - 1, PARTS)), dma((blocks, n - 1, PARTS)), dma((blocks,)),
        ],
        compiler_params=pltpu.CompilerParams(dimension_semantics=("arbitrary",), vmem_limit_bytes=VMEM, collective_id=0, has_side_effects=True),
        name="fused",
    )(x, x, gain, tab, tab, wq, wk, wv, wo)


def solution(mesh):
    def step(x, gain, wq, wk, wv, wo):
        return fused(mesh.shape["tp"], x, gain, wq, wk, wv, wo)

    tokens, columns = P("dp", None), P(None, "tp")
    return jax.shard_map(
        step,
        mesh=mesh,
        in_specs=(tokens, P(None), columns, columns, columns, P("tp", None)),
        out_specs=tokens,
        check_vma=False,
    )
```
